128 devices in a mesh: row: 8 (over y, core), col: 16 (over z, x).
Axes of the slice: x: 4, y: 4, z: 4, core: 2. Of those that a mesh axis runs over, the one named last changes fastest.
Arguments:
- matrix: float32 [8, 8, 256, 4, 16, 256], P(None, 'row', None, None, 'col'), may hold values from -10 to 20, as said below
Outputs:
- factored: float32 [8, 8, 256, 4, 16, 256], P(None, 'row', None, None, 'col')
The draws below stay inside these ranges and needn't reach their ends.
Inputs may be any that keep to these rules, and one draw needn't show every extreme that they name: matrix is symmetric, and its leading 2 * 256 rows and columns form a positive definite block.
All inputs are finite; a program needn't handle non-finite values.
Results may differ from the reference program's by a relative error of at most 0.0001.
Values sent between devices are 32-bit elements; how exact they have to be, the bound alone decides.
No kernel may reach another device: no remote copies, remote signals or barrier semaphores. Data moves between devices by JAX's collectives and lax.ppermute only.
A program may use at most 128 MiB of HBM per device.

```python
import jax
import jax.numpy as jnp
from jax import lax

N = 16384
NB = 256
STEPS = 2
KR = 8
KC = 4
N_ROW = 8
N_COL = 16


def draw_matrix(key, part):
    base = jax.random.fold_in(key, 11)
    first = jax.random.fold_in(base, 0)
    fourth = jax.random.fold_in(base, 3)
    leading = STEPS * NB
    random_part = jnp.clip(jax.random.normal(first, (N, N), jnp.float32), -4.0, 4.0)
    mixing = jnp.clip(jax.random.normal(fourth, (leading, leading), jnp.float32), -5.0, 5.0)
    symmetric = (random_part + random_part.T) * 0.7071
    gram = jnp.dot(mixing, mixing.T, precision=lax.Precision.HIGHEST) * (4.0 / leading)
    gram = (gram + gram.T) * 0.5
    dominant = gram + 4.0 * jnp.eye(leading, dtype=jnp.float32)
    symmetric = symmetric.at[:leading, :leading].set(dominant)
    return symmetric.reshape(KR, N_ROW, NB, KC, N_COL, NB)


def setup_inputs(seed: int = 0) -> dict:
    key_of = jax.random.split(jax.random.key(seed), 2)
    matrix = draw_matrix(jax.random.fold_in(key_of[1], 71), 0)
    return {"matrix": matrix}


def reference(matrix):
    full_matrix = matrix.reshape(N, N)
    identity = jnp.eye(NB, dtype=jnp.float32)
    row_index = jnp.arange(N)
    for section_at in range(STEPS):
        offset = section_at * NB
        diag_factor = jnp.linalg.cholesky(full_matrix[offset:offset + NB, offset:offset + NB])
        diag_inverse = jax.scipy.linalg.solve_triangular(diag_factor, identity, lower=True)
        factor_panel = jnp.dot(full_matrix[:, offset:offset + NB], diag_inverse.T, precision=lax.Precision.HIGHEST)
        factor_panel = jnp.where((row_index >= offset + NB)[:, None], factor_panel, jnp.zeros_like(factor_panel))
        full_matrix = full_matrix - jnp.dot(factor_panel, factor_panel.T, precision=lax.Precision.HIGHEST)
        column = factor_panel.at[offset:offset + NB].set(diag_factor)
        full_matrix = full_matrix.at[:, offset:offset + NB].set(column)
        full_matrix = full_matrix.at[offset:offset + NB, offset + NB:].set(jnp.zeros_like(full_matrix[offset:offset + NB, offset + NB:]))
    return full_matrix.reshape(matrix.shape)
```

```python
import jax
import jax.numpy as jnp
from jax import lax
from jax.experimental import pallas as pl
from jax.experimental.pallas import tpu as pltpu
from jax.sharding import PartitionSpec as P


F32 = jnp.float32
BF16 = jnp.bfloat16
NB = 256
HALF = 128
W = 512
GROUP = 8
HIGH = lax.Precision.HIGHEST
VMEM = pl.BlockSpec(memory_space=pltpu.VMEM)
AXES = ("row", "col")
NY, NK, NZ, NX = 4, 2, 4, 4
FLOPS_US = 1_000_000_000


def device(y, k, z, x):
    return (y * NK + k) * (NZ * NX) + z * NX + x


def grid_devices():
    for y in range(NY):
        for k in range(NK):
            for z in range(NZ):
                for x in range(NX):
                    yield y, k, z, x


def swap(value, y=0, k=0, z=0, x=0, only=None):
    pairs = []
    for dev in grid_devices():
        if only is None or only(*dev):
            target = (dev[0] ^ y, dev[1] ^ k, dev[2] ^ z, dev[3] ^ x)
            pairs.append((device(*dev), device(*target)))
    return lax.ppermute(value, AXES, pairs)


def scatter(value, part):
    pairs = []
    for k in range(2):
        for col in range(NZ * NX):
            row = col % (NY * NK)
            y, core = row // NK, row % NK
            z = 2 * (col // (NY * NK)) + k
            x = (col % NX) ^ part
            pairs.append((k * (NZ * NX) + col, device(y, core, z, x)))
    return lax.ppermute(value, AXES, pairs)


def nt(a, b):
    return lax.dot_general(a, b, (((1,), (1,)), ((), ())), precision=HIGH, preferred_element_type=F32)


def nn(a, b):
    return lax.dot_general(a, b, (((1,), (0,)), ((), ())), precision=HIGH, preferred_element_type=F32)


def split(value):
    hi = value.astype(BF16)
    lo = (value - hi.astype(F32)).astype(BF16)
    return hi, lo


def extract_kernel(a_ref, corner_ref, whole_ref, *part_refs):
    k = lax.axis_index("row") % NK
    x = lax.axis_index("col") % NX

    def fill(*tiles):
        for at, (i, j) in enumerate(tiles):
            corner_ref[at] = a_ref[pl.ds(i * HALF * 8 + j, HALF, stride=8), :]

    pl.when(k == x)(lambda: fill((0, 0), (1, 0), (1, 1)))
    pl.when((k != x) & (k == 0))(lambda: fill((0, 1), (1, 1), (1, 1)))
    pl.when((k != x) & (k == 1))(lambda: fill((0, 0), (0, 1), (0, 1)))
    for b in range(4):
        for h in range(2):
            value = a_ref[pl.ds(2 * b + h, NB, stride=8), :]
            whole_ref[b, :, h * HALF:(h + 1) * HALF] = value
            part_refs[b][:, h * HALF:(h + 1) * HALF] = value


def extract(view):
    shapes = [(3, HALF, HALF), (4, NB, NB)] + [(NB, NB)] * 4
    return pl.pallas_call(
        extract_kernel,
        grid=(1,),
        in_specs=[pl.BlockSpec((NB * 8, HALF), lambda i: (0, 0))],
        out_specs=[VMEM] * 6,
        out_shape=[jax.ShapeDtypeStruct(shape, F32) for shape in shapes],
        name="extract",
    )(view)


def prep_kernel(s0, s1, s2, s3, alpha, beta):
    whole = (s0[...] + s1[...]) + (s2[...] + s3[...])
    turned = whole.T
    alpha[...] = turned[:HALF]
    beta[...] = turned[HALF:]


def prep(parts):
    half = jax.ShapeDtypeStruct((HALF, NB), F32)
    return pl.pallas_call(prep_kernel, out_shape=(half, half), name="prep")(*parts)


def factor_diagonal(a_ref, m_ref, u_ref, t_ref):
    rows = lax.broadcasted_iota(jnp.int32, (HALF, HALF), 0)
    cols = lax.broadcasted_iota(jnp.int32, (HALF, HALF), 1)
    m_ref[...] = jnp.where(rows == cols, 1.0, 0.0).astype(F32)
    full = (GROUP, HALF)
    groups = HALF // GROUP
    for step in range(groups):
        base = step * GROUP
        pivot = a_ref[base:base + GROUP, :]
        for k in range(GROUP):
            t_ref[k] = jnp.broadcast_to(pivot[:, base + k:base + k + 1], full)
        s = [[None] * GROUP for _ in range(GROUP)]
        for i in range(GROUP):
            for k in range(i + 1):
                s[i][k] = jnp.broadcast_to(t_ref[k, i:i + 1, :], full)
        low = [[None] * GROUP for _ in range(GROUP)]
        inv_d = [None] * GROUP
        root = [None] * GROUP
        for k in range(GROUP):
            root[k] = lax.rsqrt(s[k][k])
            inv_d[k] = 1.0 / s[k][k]
            for i in range(k + 1, GROUP):
                low[i][k] = s[i][k] * inv_d[k]
            for i in range(k + 1, GROUP):
                for j in range(k + 1, i + 1):
                    s[i][j] = s[i][j] - low[i][k] * s[j][k]
        inv = [[None] * GROUP for _ in range(GROUP)]
        for j in range(GROUP):
            for i in range(j + 1, GROUP):
                total = low[i][j]
                for k in range(j + 1, i):
                    total = total + low[i][k] * inv[k][j]
                inv[i][j] = -total
        weights = []
        for ref, out in ((a_ref, u_ref), (m_ref, m_ref)):
            raw = [jnp.broadcast_to(ref[base + i:base + i + 1, :], full) for i in range(GROUP)]
            z = []
            for i in range(GROUP):
                total = raw[i]
                for k in range(i):
                    total = total + inv[i][k] * raw[k]
                z.append(total)
            scaled = [z[i] * inv_d[i] for i in range(GROUP)]
            w = []
            for k in range(GROUP):
                total = scaled[k]
                for i in range(k + 1, GROUP):
                    total = total + inv[i][k] * scaled[i]
                w.append(total)
            weights.append(w)
            for i in range(GROUP):
                out[base + i:base + i + 1, :] = (z[i] * root[i])[0:1, :]
        for g in range(step + 1, groups):
            at = g * GROUP
            block = a_ref[at:at + GROUP, :]
            other = m_ref[at:at + GROUP, :]
            for k in range(GROUP):
                c = jnp.broadcast_to(block[:, base + k:base + k + 1], full)
                if k == 0:
                    da = c * weights[0][0]
                    dm = c * weights[1][0]
                else:
                    da = da + c * weights[0][k]
                    dm = dm + c * weights[1][k]
            a_ref[at:at + GROUP, :] = block - da
            m_ref[at:at + GROUP, :] = other - dm


def factor_steps(first, last, s_ref, inv_ref, a_ref, m_ref, u_ref, t_ref):
    rows = lax.broadcasted_iota(jnp.int32, (HALF, HALF), 0)
    cols = lax.broadcasted_iota(jnp.int32, (HALF, HALF), 1)
    lower = rows >= cols
    zero = jnp.zeros((HALF, HALF), F32)

    def body(p, carry):
        a_ref[...] = s_ref[p, p]
        factor_diagonal(a_ref, m_ref, u_ref, t_ref)
        inverse = m_ref[...]
        s_ref[p, p] = jnp.where(lower, u_ref[...].T, 0.0)
        for q in range(first, last):

            @pl.when(p == q)
            def _(q=q):
                for j in range(q):
                    total = nn(s_ref[q, j], inv_ref[j, j])
                    for m in range(j + 1, q):
                        total = total + nn(s_ref[q, m], inv_ref[m, j])
                    inv_ref[q, j] = -nn(inverse, total)
                inv_ref[q, q] = inverse
                for j in range(q + 1, 4):
                    inv_ref[q, j] = zero
                for i in range(q + 1, 4):
                    s_ref[i, q] = nt(s_ref[i, q], inverse)
                for i in range(q + 1, 4):
                    for j in range(q + 1, i + 1):
                        s_ref[i, j] = s_ref[i, j] - nt(s_ref[i, q], s_ref[j, q])

        return carry

    lax.fori_loop(first, last, body, 0)


def chol_first_kernel(mine_ref, other_ref, s_ref, inv_ref, *work):
    k = lax.axis_index("row") % NK

    def load(top, bottom):
        s_ref[0, 0] = top[0]
        s_ref[1, 0] = top[1]
        s_ref[1, 1] = top[2]
        s_ref[2, 0] = bottom[3]
        s_ref[2, 1] = bottom[4]
        s_ref[3, 0] = top[3].T
        s_ref[3, 1] = top[4].T
        s_ref[2, 2] = bottom[0]
        s_ref[3, 2] = bottom[1]
        s_ref[3, 3] = bottom[2]

    pl.when(k == 0)(lambda: load(mine_ref, other_ref))
    pl.when(k == 1)(lambda: load(other_ref, mine_ref))
    factor_steps(0, 2, s_ref, inv_ref, *work)


def chol_last_kernel(s_in, inv_in, s_ref, inv_ref, *work):
    s_ref[...] = s_in[...]
    inv_ref[...] = inv_in[...]
    factor_steps(2, 4, s_ref, inv_ref, *work)


TILES = (4, 4, HALF, HALF)


def chol(kernel, operands, flops):
    tiles = jax.ShapeDtypeStruct(TILES, F32)
    return pl.pallas_call(
        kernel,
        in_specs=[VMEM, VMEM],
        out_specs=[VMEM, VMEM],
        out_shape=(tiles, tiles),
        cost_estimate=pl.CostEstimate(flops=flops, bytes_accessed=0, transcendentals=0),
        scratch_shapes=[
            pltpu.VMEM((HALF, HALF), F32),
            pltpu.VMEM((HALF, HALF), F32),
            pltpu.VMEM((HALF, HALF), F32),
            pltpu.VMEM((GROUP, GROUP, HALF), F32),
        ],
    )(*operands)


def three(a, b):
    return (
        jnp.dot(a[0], b[0], preferred_element_type=F32)
        + jnp.dot(a[0], b[1], preferred_element_type=F32)
        + jnp.dot(a[1], b[0], preferred_element_type=F32)
    )


def three_nt(a, b):
    def dot(u, v):
        return lax.dot_general(u, v, (((1,), (1,)), ((), ())), preferred_element_type=F32)

    return dot(a[0], b[0]) + dot(a[0], b[1]) + dot(a[1], b[0])


def finish_kernel(
    a_hbm, al0, al1, al2, al3, be0, be1, be2, be3, mine_ref, other_ref, l_ref, inv_ref,
    out_hbm, buf, lh_ref, c_ref, p_ref, pk_ref, sem_in, sem_out,
):
    row = lax.axis_index("row")
    col = lax.axis_index("col")
    k = row % NK
    z, x = col // NX, col % NX
    alphas = (al0, al1, al2, al3)
    betas = (be0, be1, be2, be3)
    size = NB * 8

    def block_of(t):
        pair, ex = t // 4, t % 4
        return ((z // 2) ^ pair) + 2 * ((x ^ ex) ^ (row % 4))

    def load(t):
        return pltpu.make_async_copy(a_hbm.at[pl.ds(block_of(t) * size, size)], buf.at[t], sem_in.at[t])

    def store(t):
        return pltpu.make_async_copy(buf.at[t], out_hbm.at[pl.ds(block_of(t) * size, size)], sem_out.at[t])

    for t in range(8):
        load(t).start()

    for i in range(4):
        for j in range(4):
            hi, lo = split(inv_ref[i, j])
            at = (slice(i * HALF, (i + 1) * HALF), slice((j % 2) * HALF, (j % 2 + 1) * HALF))
            lh_ref[(j // 2, 0) + at] = hi
            lh_ref[(j // 2, 1) + at] = lo

    def columns(top, bottom):
        for b in range(4):
            x0 = split(top[b])
            x1 = split(bottom[b])
            at = slice(b * NB, (b + 1) * NB)
            up = three((lh_ref[0, 0, :NB, :], lh_ref[0, 1, :NB, :]), x0)
            down = three((lh_ref[0, 0, NB:, :], lh_ref[0, 1, NB:, :]), x0) + three(
                (lh_ref[1, 0, NB:, :], lh_ref[1, 1, NB:, :]), x1
            )
            for i, part in enumerate((up, down)):
                hi, lo = split(part)
                c_ref[i * NB:(i + 1) * NB, at] = hi
                c_ref[W + i * NB:W + (i + 1) * NB, at] = lo
                c_ref[2 * W + i * NB:2 * W + (i + 1) * NB, at] = hi

    pl.when(k == 0)(lambda: columns(mine_ref, other_ref))
    pl.when(k == 1)(lambda: columns(other_ref, mine_ref))

    def panel(even, odd, places):
        first = z % 2
        total = three_nt(split(even), (lh_ref[first, 0], lh_ref[first, 1])) + three_nt(
            split(odd), (lh_ref[1 - first, 0], lh_ref[1 - first, 1])
        )
        for i, (t, half) in enumerate(places):
            at = slice(half * HALF, (half + 1) * HALF)
            part = total[i * HALF:(i + 1) * HALF]
            hi, lo = split(part)
            p_ref[t, at, :] = part
            pk_ref[t, at, 0:W] = hi
            pk_ref[t, at, W:2 * W] = hi
            pk_ref[t, at, 2 * W:3 * W] = lo

    for pair in range(2):
        panel(
            alphas[2 * pair][...].reshape(W, NB),
            alphas[2 * pair + 1][...].reshape(W, NB),
            [(pair * 4 + ex, 0) for ex in range(4)],
        )
    for half in range(2):
        pick = [(ex, pair) for ex in (2 * half, 2 * half + 1) for pair in range(2)]
        panel(
            jnp.concatenate([betas[ex][2 * pair] for ex, pair in pick], axis=0),
            jnp.concatenate([betas[ex][2 * pair + 1] for ex, pair in pick], axis=0),
            [(pair * 4 + ex, 1) for ex, pair in pick],
        )

    def step(u, carry):
        for m in range(2):
            load(2 * u + m).wait()
        left = pk_ref[pl.ds(2 * u, 2)].reshape(2 * NB, 3 * W)
        for b in range(4):
            update = jnp.dot(left, c_ref[:, b * NB:(b + 1) * NB], preferred_element_type=F32)
            for m in range(2):
                for h in range(2):
                    rows = pl.ds(2 * b + h, NB, stride=8)
                    part = update[m * NB:(m + 1) * NB, h * HALF:(h + 1) * HALF]
                    buf[2 * u + m, rows, :] = buf[2 * u + m, rows, :] - part

        for m in range(2):
            t = 2 * u + m
            for c in range(2):
                @pl.when(col == c)
                def _(c=c, t=t):
                    for h in range(2):
                        at = c * NB + h * HALF
                        buf[t, pl.ds(h, NB, stride=8), :] = p_ref[t, :, at:at + HALF]

            for r in range(2):
                @pl.when((row == r) & (block_of(t) == 0))
                def _(r=r, t=t):
                    for s in range(8):
                        buf[t, pl.ds(s, NB, stride=8), :] = jnp.zeros((NB, HALF), F32)
                    for c in range(r + 1):
                        @pl.when(col == c)
                        def _(c=c):
                            for i in range(2):
                                for h in range(2):
                                    if c < r or h <= i:
                                        rows = pl.ds(i * HALF * 8 + h, HALF, stride=8)
                                        buf[t, rows, :] = l_ref[2 * r + i, 2 * c + h]

            store(t).start()
        return carry

    lax.fori_loop(0, 4, step, 0)
    for t in range(8):
        store(t).wait()


def finish(view, alphas, betas, mine, other, lower, inverse):
    hbm = pl.BlockSpec(memory_space=pl.ANY)
    return pl.pallas_call(
        finish_kernel,
        in_specs=[hbm] + [VMEM] * 12,
        out_specs=hbm,
        out_shape=jax.ShapeDtypeStruct(view.shape, F32),
        scratch_shapes=[
            pltpu.VMEM((8, NB * 8, HALF), F32),
            pltpu.VMEM((2, 2, W, NB), BF16),
            pltpu.VMEM((3 * W, 4 * NB), BF16),
            pltpu.VMEM((8, NB, W), F32),
            pltpu.VMEM((8, NB, 3 * W), BF16),
            pltpu.SemaphoreType.DMA((8,)),
            pltpu.SemaphoreType.DMA((8,)),
        ],
        compiler_params=pltpu.CompilerParams(vmem_limit_bytes=56 * 1024 * 1024),
        name="finish",
    )(view, *alphas, *betas, mine, other, lower, inverse)


def after(value, *others):
    return lax.optimization_barrier((value, *others))[0]


def local(matrix):
    row = lax.axis_index("row")
    col = lax.axis_index("col")
    y, k = row // NK, row % NK
    z, x = col // NX, col % NX
    view = matrix.reshape(8 * NB * 8, HALF)

    tiles, blocks, *quarters = extract(view)
    got = [swap(tiles, y=e, only=lambda yy, kk, zz, xx: yy == 0 and zz == 0 and xx < 2) for e in (1, 3, 2)]
    parts = [scatter(quarters[b], b) for b in range(4)]

    tiles = jnp.where(y == 0, tiles, got[0] + got[1] + got[2])
    got = [swap(tiles, z=e, only=lambda yy, kk, zz, xx: zz == 0 and xx < 2) for e in (1, 3, 2)]
    tiles = jnp.where(z == 0, tiles, got[0] + got[1] + got[2])
    late = after(blocks, tiles)
    tiles = [tiles] + [swap(tiles, x=e, only=lambda yy, kk, zz, xx: xx < 2) for e in (1, 2, 3)]

    def pick(j):
        at = x ^ j
        return jnp.where(at == 0, tiles[0], jnp.where(at == 1, tiles[1], jnp.where(at == 2, tiles[2], tiles[3])))

    own = jnp.concatenate([pick(k), pick(1 - k)[:2]], axis=0)
    other = swap(own, k=1)

    alpha, beta = prep(parts)
    along_x = [alpha] + [swap(alpha, x=e) for e in (1, 2, 3)]
    along_z = [beta] + [swap(beta, z=e) for e in (1, 2, 3)]
    along_x = jnp.stack(along_x)
    along_z = jnp.stack(along_z)
    alphas = [along_x] + [swap(along_x, z=e) for e in (1, 2, 3)]
    betas = [along_z] + [swap(along_z, x=e) for e in (1, 2, 3)]

    got = [swap(late, y=e, only=lambda yy, kk, zz, xx: yy == 0) for e in (1, 2, 3)]

    own = after(own, along_x, along_z)
    lower, inverse = chol(chol_first_kernel, (own, other), 12 * FLOPS_US)
    got = lax.optimization_barrier((*got, lower))[:3]
    mine = jnp.where(y == 0, blocks, got[0] + got[1] + got[2])
    mine_other = swap(mine, k=1)
    lower = after(lower, mine)
    lower, inverse = chol(chol_last_kernel, (lower, inverse), 12 * FLOPS_US)
    out = finish(view, alphas, betas, mine, mine_other, lower, inverse)
    return out.reshape(matrix.shape)


def solution(mesh):
    spec = P(None, "row", None, None, "col", None)
    return jax.shard_map(local, mesh=mesh, in_specs=(spec,), out_specs=spec, check_vma=False)
```

```python
import jax
import jax.numpy as jnp
from jax import lax
from jax.experimental import pallas as pl
from jax.experimental.pallas import tpu as pltpu
from jax.sharding import PartitionSpec as P


F32 = jnp.float32
BF16 = jnp.bfloat16
NB = 256
HALF = 128
W = 512
GROUP = 8
HIGH = lax.Precision.HIGHEST
VMEM = pl.BlockSpec(memory_space=pltpu.VMEM)
AXES = ("row", "col")
NY, NK, NZ, NX = 4, 2, 4, 4
FLOPS_US = 1_000_000_000


def device(y, k, z, x):
    return (y * NK + k) * (NZ * NX) + z * NX + x


def grid_devices():
    for y in range(NY):
        for k in range(NK):
            for z in range(NZ):
                for x in range(NX):
                    yield y, k, z, x


def swap(value, y=0, k=0, z=0, x=0, only=None):
    pairs = []
    for dev in grid_devices():
        if only is None or only(*dev):
            target = (dev[0] ^ y, dev[1] ^ k, dev[2] ^ z, dev[3] ^ x)
            pairs.append((device(*dev), device(*target)))
    return lax.ppermute(value, AXES, pairs)


def scatter(value, part):
    pairs = []
    for k in range(2):
        for col in range(NZ * NX):
            row = col % (NY * NK)
            y, core = row // NK, row % NK
            z = 2 * (col // (NY * NK)) + k
            x = (col % NX) ^ part
            pairs.append((k * (NZ * NX) + col, device(y, core, z, x)))
    return lax.ppermute(value, AXES, pairs)


def nt(a, b):
    return lax.dot_general(a, b, (((1,), (1,)), ((), ())), precision=HIGH, preferred_element_type=F32)


def nn(a, b):
    return lax.dot_general(a, b, (((1,), (0,)), ((), ())), precision=HIGH, preferred_element_type=F32)


def split(value):
    hi = value.astype(BF16)
    lo = (value - hi.astype(F32)).astype(BF16)
    return hi, lo


def extract_kernel(a_hbm, corner_ref, whole_ref, p0_ref, p1_ref, p2_ref, p3_ref, a_ref, sem):
    part_refs = (p0_ref, p1_ref, p2_ref, p3_ref)
    copy = pltpu.make_async_copy(a_hbm.at[pl.ds(0, NB * 8)], a_ref, sem)
    copy.start()
    copy.wait()
    k = lax.axis_index("row") % NK
    x = lax.axis_index("col") % NX

    def fill(*tiles):
        for at, (i, j) in enumerate(tiles):
            corner_ref[at] = a_ref[pl.ds(i * HALF * 8 + j, HALF, stride=8), :]

    pl.when(k == x)(lambda: fill((0, 0), (1, 0), (1, 1)))
    pl.when((k != x) & (k == 0))(lambda: fill((0, 1), (1, 1), (1, 1)))
    pl.when((k != x) & (k == 1))(lambda: fill((0, 0), (0, 1), (0, 1)))
    for b in range(4):
        for h in range(2):
            value = a_ref[pl.ds(2 * b + h, NB, stride=8), :]
            whole_ref[b, :, h * HALF:(h + 1) * HALF] = value
            part_refs[b][:, h * HALF:(h + 1) * HALF] = value


def extract(view):
    shapes = [(3, HALF, HALF), (4, NB, NB)] + [(NB, NB)] * 4
    return pl.pallas_call(
        extract_kernel,
        in_specs=[pl.BlockSpec(memory_space=pltpu.HBM)],
        out_specs=[VMEM] * 6,
        scratch_shapes=[pltpu.VMEM((NB * 8, HALF), F32), pltpu.SemaphoreType.DMA],
        out_shape=[jax.ShapeDtypeStruct(shape, F32) for shape in shapes],
        compiler_params=pltpu.CompilerParams(vmem_limit_bytes=57 * 1024 * 1024),
        name="extract",
    )(view)


def prep_kernel(s0, s1, s2, s3, alpha, beta):
    whole = (s0[...] + s1[...]) + (s2[...] + s3[...])
    turned = whole.T
    alpha[...] = turned[:HALF]
    beta[...] = turned[HALF:]


def prep(parts):
    half = jax.ShapeDtypeStruct((HALF, NB), F32)
    return pl.pallas_call(
        prep_kernel,
        out_shape=(half, half),
        compiler_params=pltpu.CompilerParams(vmem_limit_bytes=4 * 1024 * 1024),
        name="prep",
    )(*parts)


def factor_diagonal(a_ref, m_ref, u_ref, t_ref):
    rows = lax.broadcasted_iota(jnp.int32, (HALF, HALF), 0)
    cols = lax.broadcasted_iota(jnp.int32, (HALF, HALF), 1)
    m_ref[:HALF] = jnp.where(rows == cols, 1.0, 0.0).astype(F32)
    full = (GROUP, HALF)
    groups = HALF // GROUP
    for step in range(groups):
        base = step * GROUP
        pivot = a_ref[base:base + GROUP, :]
        for k in range(GROUP):
            t_ref[k, :GROUP] = jnp.broadcast_to(pivot[:, base + k:base + k + 1], full)
        s = [[None] * GROUP for _ in range(GROUP)]
        for i in range(GROUP):
            for k in range(i + 1):
                s[i][k] = t_ref[k, pl.ds(i, GROUP, stride=0), :]
        low = [[None] * GROUP for _ in range(GROUP)]
        inv_d = [None] * GROUP
        root = [None] * GROUP
        for k in range(GROUP):
            root[k] = lax.rsqrt(s[k][k])
            inv_d[k] = 1.0 / s[k][k]
            for i in range(k + 1, GROUP):
                low[i][k] = s[i][k] * inv_d[k]
            for i in range(k + 1, GROUP):
                for j in range(k + 1, i + 1):
                    s[i][j] = s[i][j] - low[i][k] * s[j][k]
        inv = [[None] * GROUP for _ in range(GROUP)]
        for j in range(GROUP):
            for i in range(j + 1, GROUP):
                total = low[i][j]
                for k in range(j + 1, i):
                    total = total + low[i][k] * inv[k][j]
                inv[i][j] = -total
        weights = []
        for ref, out in ((a_ref, u_ref), (m_ref, m_ref)):
            raw = [ref[pl.ds(base + i, GROUP, stride=0), :] for i in range(GROUP)]
            z = []
            for i in range(GROUP):
                total = raw[i]
                for k in range(i):
                    total = total + inv[i][k] * raw[k]
                z.append(total)
            scaled = [z[i] * inv_d[i] for i in range(GROUP)]
            w = []
            for k in range(GROUP):
                total = scaled[k]
                for i in range(k + 1, GROUP):
                    total = total + inv[i][k] * scaled[i]
                w.append(total)
            weights.append(w)
            for i in range(GROUP):
                out[base + i:base + i + 1, :] = (z[i] * root[i])[0:1, :]
        for g in range(step + 1, groups):
            at = g * GROUP
            block = a_ref[at:at + GROUP, :]
            other = m_ref[at:at + GROUP, :]
            for k in range(GROUP):
                c = jnp.broadcast_to(block[:, base + k:base + k + 1], full)
                if k == 0:
                    da = c * weights[0][0]
                    dm = c * weights[1][0]
                else:
                    da = da + c * weights[0][k]
                    dm = dm + c * weights[1][k]
            a_ref[at:at + GROUP, :] = block - da
            m_ref[at:at + GROUP, :] = other - dm


def factor_steps(first, last, s_ref, inv_ref, a_ref, m_ref, u_ref, t_ref):
    rows = lax.broadcasted_iota(jnp.int32, (HALF, HALF), 0)
    cols = lax.broadcasted_iota(jnp.int32, (HALF, HALF), 1)
    lower = rows >= cols
    zero = jnp.zeros((HALF, HALF), F32)

    def body(p, carry):
        a_ref[:HALF] = s_ref[p, p]
        factor_diagonal(a_ref, m_ref, u_ref, t_ref)
        inverse = m_ref[:HALF]
        s_ref[p, p] = jnp.where(lower, u_ref[...].T, 0.0)
        for q in range(first, last):

            @pl.when(p == q)
            def _(q=q):
                for j in range(q):
                    total = nn(s_ref[q, j], inv_ref[j, j])
                    for m in range(j + 1, q):
                        total = total + nn(s_ref[q, m], inv_ref[m, j])
                    inv_ref[q, j] = -nn(inverse, total)
                inv_ref[q, q] = inverse
                for j in range(q + 1, 4):
                    inv_ref[q, j] = zero
                for i in range(q + 1, 4):
                    s_ref[i, q] = nt(s_ref[i, q], inverse)
                for i in range(q + 1, 4):
                    for j in range(q + 1, i + 1):
                        s_ref[i, j] = s_ref[i, j] - nt(s_ref[i, q], s_ref[j, q])

        return carry

    lax.fori_loop(first, last, body, 0)


def chol_first_kernel(mine_ref, other_ref, s_ref, inv_ref, *work):
    k = lax.axis_index("row") % NK

    def load(top, bottom):
        s_ref[0, 0] = top[0]
        s_ref[1, 0] = top[1]
        s_ref[1, 1] = top[2]
        s_ref[2, 0] = bottom[3]
        s_ref[2, 1] = bottom[4]
        s_ref[3, 0] = top[3].T
        s_ref[3, 1] = top[4].T
        s_ref[2, 2] = bottom[0]
        s_ref[3, 2] = bottom[1]
        s_ref[3, 3] = bottom[2]

    pl.when(k == 0)(lambda: load(mine_ref, other_ref))
    pl.when(k == 1)(lambda: load(other_ref, mine_ref))
    factor_steps(0, 2, s_ref, inv_ref, *work)


def chol_last_kernel(s_in, inv_in, s_ref, inv_ref, *work):
    s_ref[...] = s_in[...]
    inv_ref[...] = inv_in[...]
    factor_steps(2, 4, s_ref, inv_ref, *work)


TILES = (4, 4, HALF, HALF)


def chol(kernel, operands, flops):
    tiles = jax.ShapeDtypeStruct(TILES, F32)
    return pl.pallas_call(
        kernel,
        in_specs=[VMEM, VMEM],
        out_specs=[VMEM, VMEM],
        out_shape=(tiles, tiles),
        cost_estimate=pl.CostEstimate(flops=flops, bytes_accessed=0, transcendentals=0),
        scratch_shapes=[
            pltpu.VMEM((HALF + GROUP, HALF), F32),
            pltpu.VMEM((HALF + GROUP, HALF), F32),
            pltpu.VMEM((HALF, HALF), F32),
            pltpu.VMEM((GROUP, 2 * GROUP, HALF), F32),
        ],
        compiler_params=pltpu.CompilerParams(vmem_limit_bytes=8 * 1024 * 1024),
    )(*operands)


def three(a, b):
    return (
        jnp.dot(a[0], b[0], preferred_element_type=F32)
        + jnp.dot(a[0], b[1], preferred_element_type=F32)
        + jnp.dot(a[1], b[0], preferred_element_type=F32)
    )


def three_nt(a, b):
    def dot(u, v):
        return lax.dot_general(u, v, (((1,), (1,)), ((), ())), preferred_element_type=F32)

    return dot(a[0], b[0]) + dot(a[0], b[1]) + dot(a[1], b[0])


def finish_kernel(
    a_ref, al0, al1, al2, al3, be0, be1, be2, be3, mine_ref, other_ref, l_ref, inv_ref,
    out_hbm, buf, lh_ref, c_ref, p_ref, pk_ref, sem_out,
):
    row = lax.axis_index("row")
    col = lax.axis_index("col")
    k = row % NK
    z, x = col // NX, col % NX
    alphas = (al0, al1, al2, al3)
    betas = (be0, be1, be2, be3)
    size = NB * 8

    def block_of(t):
        pair, ex = t // 4, t % 4
        return ((z // 2) ^ pair) + 2 * ((x ^ ex) ^ (row % 4))

    def store(t):
        return pltpu.make_async_copy(buf.at[t], out_hbm.at[pl.ds(block_of(t) * size, size)], sem_out.at[t])

    for i in range(4):
        for j in range(4):
            hi, lo = split(inv_ref[i, j])
            at = (slice(i * HALF, (i + 1) * HALF), slice((j % 2) * HALF, (j % 2 + 1) * HALF))
            lh_ref[(j // 2, 0) + at] = hi
            lh_ref[(j // 2, 1) + at] = lo

    def columns(top, bottom):
        for b in range(4):
            x0 = split(top[b])
            x1 = split(bottom[b])
            at = slice(b * NB, (b + 1) * NB)
            up = three((lh_ref[0, 0, :NB, :], lh_ref[0, 1, :NB, :]), x0)
            down = three((lh_ref[0, 0, NB:, :], lh_ref[0, 1, NB:, :]), x0) + three(
                (lh_ref[1, 0, NB:, :], lh_ref[1, 1, NB:, :]), x1
            )
            for i, part in enumerate((up, down)):
                hi, lo = split(part)
                c_ref[i * NB:(i + 1) * NB, at] = hi
                c_ref[W + i * NB:W + (i + 1) * NB, at] = lo
                c_ref[2 * W + i * NB:2 * W + (i + 1) * NB, at] = hi

    pl.when(k == 0)(lambda: columns(mine_ref, other_ref))
    pl.when(k == 1)(lambda: columns(other_ref, mine_ref))

    def panel(even, odd, places):
        first = z % 2
        total = three_nt(split(even), (lh_ref[first, 0], lh_ref[first, 1])) + three_nt(
            split(odd), (lh_ref[1 - first, 0], lh_ref[1 - first, 1])
        )
        for i, (t, half) in enumerate(places):
            at = slice(half * HALF, (half + 1) * HALF)
            part = total[i * HALF:(i + 1) * HALF]
            hi, lo = split(part)
            p_ref[t, at, :] = part
            pk_ref[t, at, 0:W] = hi
            pk_ref[t, at, W:2 * W] = hi
            pk_ref[t, at, 2 * W:3 * W] = lo

    for pair in range(2):
        panel(
            alphas[2 * pair][...].reshape(W, NB),
            alphas[2 * pair + 1][...].reshape(W, NB),
            [(pair * 4 + ex, 0) for ex in range(4)],
        )
    for half in range(2):
        pick = [(ex, pair) for ex in (2 * half, 2 * half + 1) for pair in range(2)]
        panel(
            jnp.concatenate([betas[ex][2 * pair] for ex, pair in pick], axis=0),
            jnp.concatenate([betas[ex][2 * pair + 1] for ex, pair in pick], axis=0),
            [(pair * 4 + ex, 1) for ex, pair in pick],
        )

    def step(u, carry):
        left = pk_ref[pl.ds(2 * u, 2)].reshape(2 * NB, 3 * W)
        for b in range(4):
            update = jnp.dot(left, c_ref[:, b * NB:(b + 1) * NB], preferred_element_type=F32)
            for m in range(2):
                for h in range(2):
                    rows = pl.ds(2 * b + h, NB, stride=8)
                    part = update[m * NB:(m + 1) * NB, h * HALF:(h + 1) * HALF]
                    source = pl.ds(block_of(2 * u + m) * size + 2 * b + h, NB, stride=8)
                    buf[2 * u + m, rows, :] = a_ref[source, :] - part

        for m in range(2):
            t = 2 * u + m
            for c in range(2):
                @pl.when(col == c)
                def _(c=c, t=t):
                    for h in range(2):
                        at = c * NB + h * HALF
                        buf[t, pl.ds(h, NB, stride=8), :] = p_ref[t, :, at:at + HALF]

            for r in range(2):
                @pl.when((row == r) & (block_of(t) == 0))
                def _(r=r, t=t):
                    for s in range(8):
                        buf[t, pl.ds(s, NB, stride=8), :] = jnp.zeros((NB, HALF), F32)
                    for c in range(r + 1):
                        @pl.when(col == c)
                        def _(c=c):
                            for i in range(2):
                                for h in range(2):
                                    if c < r or h <= i:
                                        rows = pl.ds(i * HALF * 8 + h, HALF, stride=8)
                                        buf[t, rows, :] = l_ref[2 * r + i, 2 * c + h]

            store(t).start()
        return carry

    lax.fori_loop(0, 4, step, 0)
    for t in range(8):
        store(t).wait()


def finish(view, alphas, betas, mine, other, lower, inverse):
    hbm = pl.BlockSpec(memory_space=pl.ANY)
    return pl.pallas_call(
        finish_kernel,
        in_specs=[VMEM] * 13,
        out_specs=hbm,
        out_shape=jax.ShapeDtypeStruct(view.shape, F32),
        scratch_shapes=[
            pltpu.VMEM((8, NB * 8, HALF), F32),
            pltpu.VMEM((2, 2, W, NB), BF16),
            pltpu.VMEM((3 * W, 4 * NB), BF16),
            pltpu.VMEM((8, NB, W), F32),
            pltpu.VMEM((8, NB, 3 * W), BF16),
            pltpu.SemaphoreType.DMA((8,)),
        ],
        compiler_params=pltpu.CompilerParams(vmem_limit_bytes=28 * 1024 * 1024),
        name="finish",
    )(view, *alphas, *betas, mine, other, lower, inverse)


def after(value, *others):
    return lax.optimization_barrier((value, *others))[0]


def local(matrix):
    row = lax.axis_index("row")
    col = lax.axis_index("col")
    y, k = row // NK, row % NK
    z, x = col // NX, col % NX
    view = matrix.reshape(8 * NB * 8, HALF)

    tiles, blocks, *quarters = extract(view)
    got = [swap(tiles, y=e, only=lambda yy, kk, zz, xx: yy == 0 and zz == 0 and xx < 2) for e in (1, 3, 2)]
    parts = [scatter(quarters[b], b) for b in range(4)]

    tiles = jnp.where(y == 0, tiles, got[0] + got[1] + got[2])
    got = [swap(tiles, z=e, only=lambda yy, kk, zz, xx: zz == 0 and xx < 2) for e in (1, 3, 2)]
    tiles = jnp.where(z == 0, tiles, got[0] + got[1] + got[2])
    late = after(blocks, tiles)
    tiles = [tiles] + [swap(tiles, x=e, only=lambda yy, kk, zz, xx: xx < 2) for e in (1, 2, 3)]

    def pick(j):
        at = x ^ j
        return jnp.where(at == 0, tiles[0], jnp.where(at == 1, tiles[1], jnp.where(at == 2, tiles[2], tiles[3])))

    own = jnp.concatenate([pick(k), pick(1 - k)[:2]], axis=0)
    other = swap(own, k=1)

    alpha, beta = prep(parts)
    along_x = [alpha] + [swap(alpha, x=e) for e in (1, 2, 3)]
    along_z = [beta] + [swap(beta, z=e) for e in (1, 2, 3)]
    along_x = jnp.stack(along_x)
    along_z = jnp.stack(along_z)
    alphas = [along_x] + [swap(along_x, z=e) for e in (1, 2, 3)]
    betas = [along_z] + [swap(along_z, x=e) for e in (1, 2, 3)]

    got = [swap(late, y=e, only=lambda yy, kk, zz, xx: yy == 0) for e in (1, 2, 3)]

    own = after(own, along_x, along_z)
    lower, inverse = chol(chol_first_kernel, (own, other), 12 * FLOPS_US)
    got = lax.optimization_barrier((*got, lower))[:3]
    mine = jnp.where(y == 0, blocks, got[0] + got[1] + got[2])
    mine_other = swap(mine, k=1)
    lower = after(lower, mine)
    lower, inverse = chol(chol_last_kernel, (lower, inverse), 12 * FLOPS_US)
    out = finish(view, alphas, betas, mine, mine_other, lower, inverse)
    return out.reshape(matrix.shape)


def solution(mesh):
    spec = P(None, "row", None, None, "col", None)
    return jax.shard_map(local, mesh=mesh, in_specs=(spec,), out_specs=spec, check_vma=False)
```

```python
import jax
import jax.numpy as jnp
from jax import lax
from jax.experimental import pallas as pl
from jax.experimental.pallas import tpu as pltpu
from jax.sharding import PartitionSpec as P


F32 = jnp.float32
BF16 = jnp.bfloat16
NB = 256
HALF = 128
W = 512
GROUP = 8
HIGH = lax.Precision.HIGHEST
VMEM = pl.BlockSpec(memory_space=pltpu.VMEM)
AXES = ("row", "col")
NY, NK, NZ, NX = 4, 2, 4, 4
FLOPS_US = 1_000_000_000


def device(y, k, z, x):
    return (y * NK + k) * (NZ * NX) + z * NX + x


def grid_devices():
    for y in range(NY):
        for k in range(NK):
            for z in range(NZ):
                for x in range(NX):
                    yield y, k, z, x


def swap(value, y=0, k=0, z=0, x=0, only=None):
    pairs = []
    for dev in grid_devices():
        if only is None or only(*dev):
            target = (dev[0] ^ y, dev[1] ^ k, dev[2] ^ z, dev[3] ^ x)
            pairs.append((device(*dev), device(*target)))
    return lax.ppermute(value, AXES, pairs)


def scatter(value, part):
    pairs = []
    for k in range(2):
        for col in range(NZ * NX):
            row = col % (NY * NK)
            y, core = row // NK, row % NK
            z = 2 * (col // (NY * NK)) + k
            x = (col % NX) ^ part
            pairs.append((k * (NZ * NX) + col, device(y, core, z, x)))
    return lax.ppermute(value, AXES, pairs)


def nt(a, b):
    return lax.dot_general(a, b, (((1,), (1,)), ((), ())), precision=HIGH, preferred_element_type=F32)


def nn(a, b):
    return lax.dot_general(a, b, (((1,), (0,)), ((), ())), precision=HIGH, preferred_element_type=F32)


def split(value):
    hi = value.astype(BF16)
    lo = (value - hi.astype(F32)).astype(BF16)
    return hi, lo


def extract_kernel(a_hbm, corner_ref, whole_ref, p0_ref, p1_ref, p2_ref, p3_ref, a_ref, sem):
    part_refs = (p0_ref, p1_ref, p2_ref, p3_ref)
    copy = pltpu.make_async_copy(a_hbm.at[pl.ds(0, NB * 8)], a_ref, sem)
    copy.start()
    copy.wait()
    k = lax.axis_index("row") % NK
    x = lax.axis_index("col") % NX

    def fill(*tiles):
        for at, (i, j) in enumerate(tiles):
            corner_ref[at] = a_ref[pl.ds(i * HALF * 8 + j, HALF, stride=8), :]

    pl.when(k == x)(lambda: fill((0, 0), (1, 0), (1, 1)))
    pl.when((k != x) & (k == 0))(lambda: fill((0, 1), (1, 1), (1, 1)))
    pl.when((k != x) & (k == 1))(lambda: fill((0, 0), (0, 1), (0, 1)))
    for b in range(4):
        for h in range(2):
            value = a_ref[pl.ds(2 * b + h, NB, stride=8), :]
            whole_ref[b, :, h * HALF:(h + 1) * HALF] = value
            part_refs[b][:, h * HALF:(h + 1) * HALF] = value


def extract(view):
    shapes = [(3, HALF, HALF), (4, NB, NB)] + [(NB, NB)] * 4
    return pl.pallas_call(
        extract_kernel,
        in_specs=[pl.BlockSpec(memory_space=pltpu.HBM)],
        out_specs=[VMEM] * 6,
        scratch_shapes=[pltpu.VMEM((NB * 8, HALF), F32), pltpu.SemaphoreType.DMA],
        out_shape=[jax.ShapeDtypeStruct(shape, F32) for shape in shapes],
        compiler_params=pltpu.CompilerParams(vmem_limit_bytes=57 * 1024 * 1024),
        name="extract",
    )(view)


def prep_kernel(s0, s1, s2, s3, alpha, beta):
    whole = (s0[...] + s1[...]) + (s2[...] + s3[...])
    turned = whole.T
    alpha[...] = turned[:HALF]
    beta[...] = turned[HALF:]


def prep(parts):
    half = jax.ShapeDtypeStruct((HALF, NB), F32)
    return pl.pallas_call(
        prep_kernel,
        out_shape=(half, half),
        compiler_params=pltpu.CompilerParams(vmem_limit_bytes=4 * 1024 * 1024),
        name="prep",
    )(*parts)


def factor_diagonal(a_ref, m_ref, u_ref, t_ref):
    rows = lax.broadcasted_iota(jnp.int32, (HALF, HALF), 0)
    cols = lax.broadcasted_iota(jnp.int32, (HALF, HALF), 1)
    m_ref[:HALF] = jnp.where(rows == cols, 1.0, 0.0).astype(F32)
    full = (GROUP, HALF)
    groups = HALF // GROUP
    for step in range(groups):
        base = step * GROUP
        pivot = a_ref[base:base + GROUP, :]
        for k in range(GROUP):
            t_ref[k, :GROUP] = jnp.broadcast_to(pivot[:, base + k:base + k + 1], full)
        s = [[None] * GROUP for _ in range(GROUP)]
        for i in range(GROUP):
            for k in range(i + 1):
                s[i][k] = t_ref[k, pl.ds(i, GROUP, stride=0), :]
        low = [[None] * GROUP for _ in range(GROUP)]
        inv_d = [None] * GROUP
        root = [None] * GROUP
        for k in range(GROUP):
            root[k] = lax.rsqrt(s[k][k])
            inv_d[k] = 1.0 / s[k][k]
            for i in range(k + 1, GROUP):
                low[i][k] = s[i][k] * inv_d[k]
            for i in range(k + 1, GROUP):
                for j in range(k + 1, i + 1):
                    s[i][j] = s[i][j] - low[i][k] * s[j][k]
        inv = [[None] * GROUP for _ in range(GROUP)]
        for j in range(GROUP):
            for i in range(j + 1, GROUP):
                total = low[i][j]
                for k in range(j + 1, i):
                    total = total + low[i][k] * inv[k][j]
                inv[i][j] = -total
        weights = []
        for ref, out in ((a_ref, u_ref), (m_ref, m_ref)):
            raw = [ref[pl.ds(base + i, GROUP, stride=0), :] for i in range(GROUP)]
            z = []
            for i in range(GROUP):
                total = raw[i]
                for k in range(i):
                    total = total + inv[i][k] * raw[k]
                z.append(total)
            scaled = [z[i] * inv_d[i] for i in range(GROUP)]
            w = []
            for k in range(GROUP):
                total = scaled[k]
                for i in range(k + 1, GROUP):
                    total = total + inv[i][k] * scaled[i]
                w.append(total)
            weights.append(w)
            for i in range(GROUP):
                out[base + i:base + i + 1, :] = (z[i] * root[i])[0:1, :]
        for g in range(step + 1, groups):
            at = g * GROUP
            block = a_ref[at:at + GROUP, :]
            other = m_ref[at:at + GROUP, :]
            for k in range(GROUP):
                c = jnp.broadcast_to(block[:, base + k:base + k + 1], full)
                if k == 0:
                    da = c * weights[0][0]
                    dm = c * weights[1][0]
                else:
                    da = da + c * weights[0][k]
                    dm = dm + c * weights[1][k]
            a_ref[at:at + GROUP, :] = block - da
            m_ref[at:at + GROUP, :] = other - dm


def factor_steps(first, last, s_ref, inv_ref, a_ref, m_ref, u_ref, t_ref):
    rows = lax.broadcasted_iota(jnp.int32, (HALF, HALF), 0)
    cols = lax.broadcasted_iota(jnp.int32, (HALF, HALF), 1)
    lower = rows >= cols
    zero = jnp.zeros((HALF, HALF), F32)

    def body(p, carry):
        a_ref[:HALF] = s_ref[p, p]
        factor_diagonal(a_ref, m_ref, u_ref, t_ref)
        inverse = m_ref[:HALF]
        s_ref[p, p] = jnp.where(lower, u_ref[...].T, 0.0)
        for q in range(first, last):

            @pl.when(p == q)
            def _(q=q):
                for j in range(q):
                    total = nn(s_ref[q, j], inv_ref[j, j])
                    for m in range(j + 1, q):
                        total = total + nn(s_ref[q, m], inv_ref[m, j])
                    inv_ref[q, j] = -nn(inverse, total)
                inv_ref[q, q] = inverse
                for j in range(q + 1, 4):
                    inv_ref[q, j] = zero
                for i in range(q + 1, 4):
                    s_ref[i, q] = nt(s_ref[i, q], inverse)
                for i in range(q + 1, 4):
                    for j in range(q + 1, i + 1):
                        s_ref[i, j] = s_ref[i, j] - nt(s_ref[i, q], s_ref[j, q])

        return carry

    lax.fori_loop(first, last, body, 0)


def chol_first_kernel(mine_ref, other_ref, s_ref, inv_ref, *work):
    k = lax.axis_index("row") % NK

    def load(top, bottom):
        s_ref[0, 0] = top[0]
        s_ref[1, 0] = top[1]
        s_ref[1, 1] = top[2]
        s_ref[2, 0] = bottom[3]
        s_ref[2, 1] = bottom[4]
        s_ref[3, 0] = top[3].T
        s_ref[3, 1] = top[4].T
        s_ref[2, 2] = bottom[0]
        s_ref[3, 2] = bottom[1]
        s_ref[3, 3] = bottom[2]

    pl.when(k == 0)(lambda: load(mine_ref, other_ref))
    pl.when(k == 1)(lambda: load(other_ref, mine_ref))
    factor_steps(0, 3, s_ref, inv_ref, *work)


def chol_last_kernel(s_in, inv_in, s_ref, inv_ref, *work):
    s_ref[...] = s_in[...]
    inv_ref[...] = inv_in[...]
    factor_steps(3, 4, s_ref, inv_ref, *work)


TILES = (4, 4, HALF, HALF)


def chol(kernel, operands, flops):
    tiles = jax.ShapeDtypeStruct(TILES, F32)
    return pl.pallas_call(
        kernel,
        in_specs=[VMEM, VMEM],
        out_specs=[VMEM, VMEM],
        out_shape=(tiles, tiles),
        cost_estimate=pl.CostEstimate(flops=flops, bytes_accessed=0, transcendentals=0),
        scratch_shapes=[
            pltpu.VMEM((HALF + GROUP, HALF), F32),
            pltpu.VMEM((HALF + GROUP, HALF), F32),
            pltpu.VMEM((HALF, HALF), F32),
            pltpu.VMEM((GROUP, 2 * GROUP, HALF), F32),
        ],
        compiler_params=pltpu.CompilerParams(vmem_limit_bytes=8 * 1024 * 1024),
    )(*operands)


def three(a, b):
    return (
        jnp.dot(a[0], b[0], preferred_element_type=F32)
        + jnp.dot(a[0], b[1], preferred_element_type=F32)
        + jnp.dot(a[1], b[0], preferred_element_type=F32)
    )


def three_nt(a, b):
    def dot(u, v):
        return lax.dot_general(u, v, (((1,), (1,)), ((), ())), preferred_element_type=F32)

    return dot(a[0], b[0]) + dot(a[0], b[1]) + dot(a[1], b[0])


def finish_kernel(
    a_ref, al0, al1, al2, al3, be0, be1, be2, be3, mine_ref, other_ref, l_ref, inv_ref,
    out_hbm, buf, lh_ref, c_ref, p_ref, pk_ref, sem_out,
):
    row = lax.axis_index("row")
    col = lax.axis_index("col")
    k = row % NK
    z, x = col // NX, col % NX
    alphas = (al0, al1, al2, al3)
    betas = (be0, be1, be2, be3)
    size = NB * 8

    def block_of(t):
        pair, ex = t // 4, t % 4
        return ((z // 2) ^ pair) + 2 * ((x ^ ex) ^ (row % 4))

    def store(t):
        return pltpu.make_async_copy(buf.at[t], out_hbm.at[pl.ds(block_of(t) * size, size)], sem_out.at[t])

    for i in range(4):
        for j in range(4):
            hi, lo = split(inv_ref[i, j])
            at = (slice(i * HALF, (i + 1) * HALF), slice((j % 2) * HALF, (j % 2 + 1) * HALF))
            lh_ref[(j // 2, 0) + at] = hi
            lh_ref[(j // 2, 1) + at] = lo

    def columns(top, bottom):
        for b in range(4):
            x0 = split(top[b])
            x1 = split(bottom[b])
            at = slice(b * NB, (b + 1) * NB)
            up = three((lh_ref[0, 0, :NB, :], lh_ref[0, 1, :NB, :]), x0)
            down = three((lh_ref[0, 0, NB:, :], lh_ref[0, 1, NB:, :]), x0) + three(
                (lh_ref[1, 0, NB:, :], lh_ref[1, 1, NB:, :]), x1
            )
            for i, part in enumerate((up, down)):
                hi, lo = split(part)
                c_ref[i * NB:(i + 1) * NB, at] = hi
                c_ref[W + i * NB:W + (i + 1) * NB, at] = lo
                c_ref[2 * W + i * NB:2 * W + (i + 1) * NB, at] = hi

    pl.when(k == 0)(lambda: columns(mine_ref, other_ref))
    pl.when(k == 1)(lambda: columns(other_ref, mine_ref))

    def panel(left, right, places):
        def tile(h, i):
            at = slice(i * NB, (i + 1) * NB)
            return lh_ref[h, 0, at], lh_ref[h, 1, at]

        left, right = split(left), split(right)
        up = three_nt(left, tile(0, 0))
        down = three_nt(left, tile(0, 1)) + three_nt(right, tile(1, 1))
        total = jnp.concatenate([up, down], axis=1)
        for i, (t, half) in enumerate(places):
            at = slice(half * HALF, (half + 1) * HALF)
            part = total[i * HALF:(i + 1) * HALF]
            hi, lo = split(part)
            p_ref[t, at, :] = part
            pk_ref[t, at, 0:W] = hi
            pk_ref[t, at, W:2 * W] = hi
            pk_ref[t, at, 2 * W:3 * W] = lo

    def panels(first):
        for pair in range(2):
            ez = 2 * pair + first
            panel(
                alphas[ez][...].reshape(W, NB),
                alphas[ez ^ 1][...].reshape(W, NB),
                [(pair * 4 + ex, 0) for ex in range(4)],
            )
        for half in range(2):
            pick = [(ex, pair) for ex in (2 * half, 2 * half + 1) for pair in range(2)]
            panel(
                jnp.concatenate([betas[ex][2 * pair + first] for ex, pair in pick], axis=0),
                jnp.concatenate([betas[ex][2 * pair + (1 - first)] for ex, pair in pick], axis=0),
                [(pair * 4 + ex, 1) for ex, pair in pick],
            )

    pl.when(z % 2 == 0)(lambda: panels(0))
    pl.when(z % 2 == 1)(lambda: panels(1))

    def step(u, carry):
        left = pk_ref[pl.ds(2 * u, 2)].reshape(2 * NB, 3 * W)
        for b in range(4):
            update = jnp.dot(left, c_ref[:, b * NB:(b + 1) * NB], preferred_element_type=F32)
            for m in range(2):
                for h in range(2):
                    rows = pl.ds(2 * b + h, NB, stride=8)
                    part = update[m * NB:(m + 1) * NB, h * HALF:(h + 1) * HALF]
                    source = pl.ds(block_of(2 * u + m) * size + 2 * b + h, NB, stride=8)
                    buf[2 * u + m, rows, :] = a_ref[source, :] - part

        for m in range(2):
            t = 2 * u + m
            for c in range(2):
                @pl.when(col == c)
                def _(c=c, t=t):
                    for h in range(2):
                        at = c * NB + h * HALF
                        buf[t, pl.ds(h, NB, stride=8), :] = p_ref[t, :, at:at + HALF]

            for r in range(2):
                @pl.when((row == r) & (block_of(t) == 0))
                def _(r=r, t=t):
                    for s in range(8):
                        buf[t, pl.ds(s, NB, stride=8), :] = jnp.zeros((NB, HALF), F32)
                    for c in range(r + 1):
                        @pl.when(col == c)
                        def _(c=c):
                            for i in range(2):
                                for h in range(2):
                                    if c < r or h <= i:
                                        rows = pl.ds(i * HALF * 8 + h, HALF, stride=8)
                                        buf[t, rows, :] = l_ref[2 * r + i, 2 * c + h]

            store(t).start()
        return carry

    lax.fori_loop(0, 4, step, 0)
    for t in range(8):
        store(t).wait()


def finish(view, alphas, betas, mine, other, lower, inverse):
    hbm = pl.BlockSpec(memory_space=pl.ANY)
    return pl.pallas_call(
        finish_kernel,
        in_specs=[VMEM] * 13,
        out_specs=hbm,
        out_shape=jax.ShapeDtypeStruct(view.shape, F32),
        scratch_shapes=[
            pltpu.VMEM((8, NB * 8, HALF), F32),
            pltpu.VMEM((2, 2, W, NB), BF16),
            pltpu.VMEM((3 * W, 4 * NB), BF16),
            pltpu.VMEM((8, NB, W), F32),
            pltpu.VMEM((8, NB, 3 * W), BF16),
            pltpu.SemaphoreType.DMA((8,)),
        ],
        compiler_params=pltpu.CompilerParams(vmem_limit_bytes=28 * 1024 * 1024),
        name="finish",
    )(view, *alphas, *betas, mine, other, lower, inverse)


def after(value, *others):
    return lax.optimization_barrier((value, *others))[0]


def local(matrix):
    row = lax.axis_index("row")
    col = lax.axis_index("col")
    y, k = row // NK, row % NK
    z, x = col // NX, col % NX
    view = matrix.reshape(8 * NB * 8, HALF)

    tiles, blocks, *quarters = extract(view)
    got = [swap(tiles, y=e, only=lambda yy, kk, zz, xx: yy == 0 and zz == 0 and xx < 2) for e in (1, 3, 2)]
    parts = [scatter(quarters[b], b) for b in range(4)]

    tiles = jnp.where(y == 0, tiles, got[0] + got[1] + got[2])
    got = [swap(tiles, z=e, only=lambda yy, kk, zz, xx: zz == 0 and xx < 2) for e in (1, 3, 2)]
    tiles = jnp.where(z == 0, tiles, got[0] + got[1] + got[2])
    late = after(blocks, tiles)
    tiles = [tiles] + [swap(tiles, x=e, only=lambda yy, kk, zz, xx: xx < 2) for e in (1, 2, 3)]

    def pick(j):
        at = x ^ j
        return jnp.where(at == 0, tiles[0], jnp.where(at == 1, tiles[1], jnp.where(at == 2, tiles[2], tiles[3])))

    own = jnp.concatenate([pick(k), pick(1 - k)[:2]], axis=0)
    other = swap(own, k=1)

    alpha, beta = prep(parts)
    along_x = [alpha] + [swap(alpha, x=e) for e in (1, 2, 3)]
    along_z = [beta] + [swap(beta, z=e) for e in (1, 2, 3)]
    along_x = jnp.stack(along_x)
    along_z = jnp.stack(along_z)
    alphas = [along_x] + [swap(along_x, z=e) for e in (1, 2, 3)]
    betas = [along_z] + [swap(along_z, x=e) for e in (1, 2, 3)]

    got = [swap(late, y=e, only=lambda yy, kk, zz, xx: yy == 0) for e in (1, 2, 3)]

    own = after(own, along_x, along_z)
    lower, inverse = chol(chol_first_kernel, (own, other), 15 * FLOPS_US)
    got = lax.optimization_barrier((*got, lower))[:3]
    mine = jnp.where(y == 0, blocks, got[0] + got[1] + got[2])
    mine_other = swap(mine, k=1)
    lower = after(lower, mine)
    lower, inverse = chol(chol_last_kernel, (lower, inverse), 5 * FLOPS_US)
    out = finish(view, alphas, betas, mine, mine_other, lower, inverse)
    return out.reshape(matrix.shape)


def solution(mesh):
    spec = P(None, "row", None, None, "col", None)
    return jax.shard_map(local, mesh=mesh, in_specs=(spec,), out_specs=spec, check_vma=False)
```
